32 devices in a mesh: seq: 16 (over z, y, core), ch: 2 (over x).
Axes of the slice: x: 2, y: 2, z: 4, core: 2. Of those that a mesh axis runs over, the one named last changes fastest.
Arguments:
- query_gate: bfloat16 [2, 2048, 2048], P('ch', 'seq'), may hold values from -6 to 6
- key_input: bfloat16 [2, 2048, 2048], P('ch', 'seq'), may hold values from -6 to 6
- value_input: bfloat16 [2, 2048, 2048], P('ch', 'seq'), may hold values from -6 to 6
- grad_output: bfloat16 [2, 2048, 2048], P('ch', 'seq'), may hold values from -6 to 6
- filter_raw: bfloat16 [2048, 2048], P('seq'), may hold values from -6 to 6
- skip_gain: float32 [2048], replicated, may hold values from 0.5 to 1.5
Outputs:
- grad_query: bfloat16 [2, 2048, 2048], P('ch', 'seq')
- grad_key: bfloat16 [2, 2048, 2048], P('ch', 'seq')
- grad_value: bfloat16 [2, 2048, 2048], P('ch', 'seq')
- grad_filter: float32 [2048, 2048], P('seq', 'ch')
The draws below stay inside these ranges and needn't reach their ends.
All inputs are finite; a program needn't handle non-finite values.
Results may differ from the reference program's by a relative error of at most 0.001.
Values sent between devices are 32-bit elements; how exact they have to be, the bound alone decides.
A program may use at most 128 MiB of HBM per device.

```python
import jax
import jax.numpy as jnp
from jax import lax

CHANNELS = 2048
SEQ_LEN = 2048
BATCH = 2


def block_levels(stream_key, extent, cuts, smallest, high):
    def one(axis_at, parts):
        draws = jax.random.uniform(jax.random.fold_in(jax.random.fold_in(stream_key, 6), axis_at), (parts,), jnp.float32, smallest / len(cuts), high / len(cuts))
        return jnp.repeat(jnp.exp(draws), extent[axis_at] // parts).reshape((-1,) + (1,) * (len(extent) - axis_at - 1))

    loudness = one(*cuts[0])
    for cut in cuts[1:]:
        loudness = loudness * one(*cut)
    return loudness


def gaussian(rng, dims, deviation, most, cuts=(), dtype=jnp.bfloat16):
    drawn = deviation * jax.random.normal(rng, dims, jnp.float32)
    if cuts:
        drawn = drawn * block_levels(rng, dims, cuts, -0.22, 0.18)
    return jnp.clip(drawn, -most, most).astype(dtype)


def setup_inputs(seed: int = 0) -> dict:
    key_list = jax.random.split(jax.random.key(seed), 7)
    return {
        "query_gate": gaussian(key_list[0], (BATCH, SEQ_LEN, CHANNELS), 1.0, 6.0, ((0, 2), (1, 16))),
        "key_input": gaussian(key_list[1], (BATCH, SEQ_LEN, CHANNELS), 1.0, 6.0, ((0, 2), (1, 16))),
        "value_input": gaussian(key_list[2], (BATCH, SEQ_LEN, CHANNELS), 1.0, 6.0, ((0, 2), (1, 16))),
        "grad_output": gaussian(key_list[3], (BATCH, SEQ_LEN, CHANNELS), 1.0, 6.0, ((0, 2), (1, 16))),
        "filter_raw": gaussian(key_list[4], (SEQ_LEN, CHANNELS), 1.0, 6.0, ((0, 16),)),
        "skip_gain": jnp.clip(jax.random.uniform(key_list[5], (CHANNELS,), jnp.float32, 0.5, 1.5), 0.5, 1.5),
    }


def block_grads(pieces):
    query_gate, key_input, value_input, grad_output, filter_raw, skip_gain = pieces
    length = 2 * SEQ_LEN
    filter_taps = filter_raw.astype(jnp.float32) * (SEQ_LEN ** -0.5)
    filter_spec = jnp.fft.rfft(filter_taps, n=length, axis=0)
    grads_query = []
    grads_key = []
    grads_value = []
    corr_total = jnp.zeros(filter_taps.shape, jnp.float32)
    for seq_index in range(BATCH):
        key_f = key_input[seq_index].astype(jnp.float32)
        value_f = value_input[seq_index].astype(jnp.float32)
        out_f = grad_output[seq_index].astype(jnp.float32)
        query_f = query_gate[seq_index].astype(jnp.float32)
        mixed_signal = key_f * value_f
        gated_grad = out_f * query_f
        mixed_spec = jnp.fft.rfft(mixed_signal, n=length, axis=0)
        gated_spec = jnp.fft.rfft(gated_grad, n=length, axis=0)
        conv_out = jnp.fft.irfft(mixed_spec * filter_spec, n=length, axis=0)[:SEQ_LEN] + skip_gain * mixed_signal
        back_grad = jnp.fft.irfft(jnp.conj(filter_spec) * gated_spec, n=length, axis=0)[:SEQ_LEN] + skip_gain * gated_grad
        corr_grad = jnp.fft.irfft(jnp.conj(mixed_spec) * gated_spec, n=length, axis=0)[:SEQ_LEN]
        grads_query.append((out_f * conv_out).astype(jnp.bfloat16))
        grads_key.append((back_grad * value_f).astype(jnp.bfloat16))
        grads_value.append((back_grad * key_f).astype(jnp.bfloat16))
        corr_total = corr_total + corr_grad
    return (jnp.stack(grads_query), jnp.stack(grads_key), jnp.stack(grads_value),
            corr_total * (SEQ_LEN ** -0.5))


def reference(query_gate, key_input, value_input, grad_output, filter_raw, skip_gain):
    channel_width = CHANNELS
    block_size = 256 if channel_width % 256 == 0 else channel_width
    groups = channel_width // block_size

    def split_channels(tensor_in):
        reshaped = tensor_in.reshape(tensor_in.shape[:-1] + (groups, block_size))
        return jnp.moveaxis(reshaped, -2, 0)

    def join_channels(tensor_in):
        reshaped = jnp.moveaxis(tensor_in, 0, -2)
        return reshaped.reshape(reshaped.shape[:-2] + (channel_width,))

    stacked = (split_channels(query_gate), split_channels(key_input), split_channels(value_input),
               split_channels(grad_output), split_channels(filter_raw), split_channels(skip_gain))
    results = lax.map(block_grads, stacked)
    return (join_channels(results[0]), join_channels(results[1]), join_channels(results[2]),
            join_channels(results[3]))
```

```python
import math

import numpy as np

import jax
import jax.numpy as jnp
from jax import lax
from jax.experimental import pallas as pl
from jax.experimental.pallas import tpu as pltpu
from jax.sharding import PartitionSpec as P


def angle_table(row_index, col_index, modulus):
    turn_count = row_index[:, None] * col_index[None, :] % modulus
    angles = turn_count.astype(jnp.float32) * (2.0 * math.pi / modulus)
    return (jnp.cos(angles), jnp.sin(angles))


def contract(pattern, table, operand):
    return jnp.einsum(
        pattern, table, operand, precision=lax.Precision.HIGHEST, preferred_element_type=jnp.float32
    )


def rotate(pattern, cos_table, sin_table, sense_sign, real_part, imag_part, want_imag):
    if imag_part is None:
        cos_term = contract(pattern, cos_table, real_part)
        return (cos_term, sense_sign * contract(pattern, sin_table, real_part))
    real_out = contract(pattern, cos_table, real_part) - sense_sign * contract(
        pattern, sin_table, imag_part
    )
    if not want_imag:
        return (real_out, None)
    imag_out = contract(pattern, cos_table, imag_part) + sense_sign * contract(
        pattern, sin_table, real_part
    )
    return (real_out, imag_out)


def twist(cos_table, sin_table, sense_sign, real_part, imag_part):
    return (
        real_part * cos_table - sense_sign * imag_part * sin_table,
        imag_part * cos_table + sense_sign * real_part * sin_table,
    )


def spectral_terms(z_real, z_imag, g_real, g_imag, h_real, h_imag):
    conv_real = z_real * h_real - z_imag * h_imag
    conv_imag = z_real * h_imag + z_imag * h_real
    back_real = h_real * g_real + h_imag * g_imag
    back_imag = h_real * g_imag - h_imag * g_real
    corr_real = z_real * g_real + z_imag * g_imag
    corr_imag = z_real * g_imag - z_imag * g_real
    return (conv_real - back_imag, conv_imag + back_real, corr_real, corr_imag)


def shards(query_gate, key_input, value_input, grad_output, filter_raw, skip_gain):
    seq_count = lax.axis_size("seq")
    key_f = key_input[0].astype(jnp.float32)
    value_f = value_input[0].astype(jnp.float32)
    out_f = grad_output[0].astype(jnp.float32)
    mixed = key_f * value_f
    gated = out_f * query_gate[0].astype(jnp.float32)
    tokens, channels = mixed.shape
    seq_length = tokens * seq_count
    full_length = 2 * seq_length
    inverse_scale = 1.0 / full_length
    filter_taps = filter_raw.astype(jnp.float32) * seq_length ** (-0.5)
    freq_one = jnp.arange(2 * seq_count, dtype=jnp.int32)
    block_index = jnp.arange(seq_count, dtype=jnp.int32)
    offset_index = jnp.arange(tokens, dtype=jnp.int32)
    cos_one, sin_one = angle_table(freq_one, block_index, 2 * seq_count)
    cos_inv, sin_inv = angle_table(block_index, freq_one, 2 * seq_count)
    cos_two, sin_two = angle_table(offset_index, offset_index, tokens)
    local_width = channels // seq_count
    arrived = (
        lax.all_to_all(mixed.T, "seq", split_axis=0, concat_axis=1, tiled=True),
        lax.all_to_all(gated.T, "seq", split_axis=0, concat_axis=1, tiled=True),
        lax.all_to_all(filter_taps.T, "seq", split_axis=0, concat_axis=1, tiled=True),
    )
    cos_tw, sin_tw = angle_table(freq_one, offset_index, full_length)
    spectra = []
    for line_data in arrived:
        lines = line_data.reshape(local_width, seq_count, tokens)
        real_part, imag_part = rotate("kn,cnm->ckm", cos_one, sin_one, -1.0, lines, None, True)
        real_part, imag_part = twist(cos_tw, sin_tw, -1.0, real_part, imag_part)
        spectra.append(rotate("jm,ckm->ckj", cos_two, sin_two, -1.0, real_part, imag_part, True))
    packed_real, packed_imag, corr_real, corr_imag = spectral_terms(
        spectra[0][0], spectra[0][1], spectra[1][0], spectra[1][1], spectra[2][0], spectra[2][1]
    )
    pr_mid, pi_mid = rotate("mj,ckj->ckm", cos_two, sin_two, 1.0, packed_real, packed_imag, True)
    pr_mid, pi_mid = twist(cos_tw, sin_tw, 1.0, pr_mid, pi_mid)
    cr_mid, ci_mid = rotate("mj,ckj->ckm", cos_two, sin_two, 1.0, corr_real, corr_imag, True)
    cr_mid, ci_mid = twist(cos_tw, sin_tw, 1.0, cr_mid, ci_mid)
    conv_lines, back_lines = rotate("nk,ckm->cnm", cos_inv, sin_inv, 1.0, pr_mid, pi_mid, True)
    corr_lines = rotate("nk,ckm->cnm", cos_inv, sin_inv, 1.0, cr_mid, ci_mid, False)[0]
    conv_lines = (conv_lines * inverse_scale).reshape(local_width, seq_length)
    back_lines = (back_lines * inverse_scale).reshape(local_width, seq_length)
    corr_lines = (corr_lines * inverse_scale).reshape(local_width, seq_length)
    returned = (
        lax.all_to_all(conv_lines, "seq", split_axis=1, concat_axis=0, tiled=True),
        lax.all_to_all(back_lines, "seq", split_axis=1, concat_axis=0, tiled=True),
        lax.all_to_all(corr_lines, "seq", split_axis=1, concat_axis=0, tiled=True),
    )
    conv_time = returned[0].T
    back_time = returned[1].T
    corr_time = returned[2].T
    conv_full = conv_time + skip_gain * mixed
    back_full = back_time + skip_gain * gated
    grad_query = (out_f * conv_full).astype(jnp.bfloat16)[None]
    grad_key = (back_full * value_f).astype(jnp.bfloat16)[None]
    grad_value = (back_full * key_f).astype(jnp.bfloat16)[None]
    grad_filter = lax.psum_scatter(
        corr_time * seq_length ** (-0.5), "ch", scatter_dimension=1, tiled=True
    )
    return (grad_query, grad_key, grad_value, grad_filter)


LANES = 128
VMEM_LIMIT = 60 * 1024 * 1024


def times_root(pair, turn, size):
    real, imag = pair
    turn %= size
    if turn == 0:
        return pair
    if 4 * turn == size:
        return (-imag, real)
    if 2 * turn == size:
        return (-real, -imag)
    if 4 * turn == 3 * size:
        return (imag, -real)
    cosine = math.cos(2.0 * math.pi * turn / size)
    sine = math.sin(2.0 * math.pi * turn / size)
    return (real * cosine - imag * sine, real * sine + imag * cosine)


def complex_dft(values, sense):
    size = len(values)
    if size == 1:
        return values
    even = complex_dft(values[0::2], sense)
    odd = complex_dft(values[1::2], sense)
    low, high = [], []
    for k in range(size // 2):
        er, ei = even[k]
        tr, ti = times_root(odd[k], sense * k, size)
        low.append((er + tr, ei + ti))
        high.append((er - tr, ei - ti))
    return low + high


def half_spectrum(values, size):
    if size == 2:
        return [(values[0] + values[1], None), (values[0] - values[1], None)]
    half, quarter = size // 2, size // 4
    if len(values) == half:
        total, difference = values, values
    else:
        total = [values[n] + values[n + half] for n in range(half)]
        difference = [values[n] - values[n + half] for n in range(half)]
    out = [None] * (half + 1)
    out[0::2] = half_spectrum(total, half)
    turned = [times_root((difference[n], -difference[n + quarter]), -n, size) for n in range(quarter)]
    for index, (real, imag) in enumerate(complex_dft(turned, -1)):
        k = 1 + 4 * index
        if k <= half:
            out[k] = (real, imag)
        else:
            out[size - k] = (real, -imag)
    return out


def real_from_half(terms, size, first_half):
    if size == 2:
        return [terms[0][0] + terms[1][0], terms[0][0] - terms[1][0]]
    half, quarter = size // 2, size // 4
    even = real_from_half(terms[0::2], half, False)
    chosen = []
    for index in range(quarter):
        k = 1 + 4 * index
        if k <= half:
            chosen.append(terms[k])
        else:
            real, imag = terms[size - k]
            chosen.append((real, -imag))
    turned = [times_root(pair, n, size) for n, pair in enumerate(complex_dft(chosen, 1))]
    odd = [pair[0] for pair in turned] + [-pair[1] for pair in turned]
    out = [even[n] + odd[n] for n in range(half)]
    if first_half:
        return out
    return out + [even[n] - odd[n] for n in range(half)]


def split_bf16(value):
    high = value.astype(jnp.bfloat16)
    return high, (value - high.astype(jnp.float32)).astype(jnp.bfloat16)


def three_dot(table_high, table_low, value):
    high, low = split_bf16(value)
    dot = lambda a, b: jnp.dot(a, b, preferred_element_type=jnp.float32)
    return dot(table_high, high) + (dot(table_high, low) + dot(table_low, high))


def fft_kernel(seq_count, tokens, pair_ref, taps_ref, fwd_ref, inv_ref, tw_ref, out_pair_ref, out_corr_ref, spec_ref, taps_scr, corr_scr):
    half_lanes = LANES // 2
    half_tokens = tokens // 2
    size = 2 * seq_count

    def spread_taps(block, carry):
        packed = taps_ref[block]
        rolled = pltpu.roll(packed, half_lanes, 1)
        lane = lax.broadcasted_iota(jnp.int32, packed.shape, 1)
        left = lane < half_lanes
        taps_scr[block, :half_tokens, :] = jnp.where(left, packed, rolled)
        taps_scr[block, half_tokens:, :] = jnp.where(left, rolled, packed)
        return carry

    lax.fori_loop(0, seq_count, spread_taps, 0)

    def analyse(chunk, carry):
        rows = pl.ds(pl.multiple_of(chunk * 8, 8), 8)
        for signal in range(3):
            lanes = slice(signal * LANES, (signal + 1) * LANES)
            if signal < 2:
                values = [pair_ref[signal, n, rows, :] for n in range(seq_count)]
            else:
                values = [taps_scr[n, rows, :] for n in range(seq_count)]
            for k, (real, imag) in enumerate(half_spectrum(values, size)):
                spec_ref[k, 0, rows, lanes] = real
                spec_ref[k, 1, rows, lanes] = jnp.zeros_like(real) if imag is None else imag
        return carry

    lax.fori_loop(0, tokens // 8, analyse, 0)

    fwd_high, fwd_low = fwd_ref[0], fwd_ref[1]
    inv_high, inv_low = inv_ref[0], inv_ref[1]

    def middle(k, carry):
        cosine = jnp.concatenate([tw_ref[k, 0]] * 3, axis=1)
        sine = jnp.concatenate([tw_ref[k, 1]] * 3, axis=1)
        real, imag = spec_ref[k, 0], spec_ref[k, 1]
        turned = jnp.concatenate([real * cosine + imag * sine, imag * cosine - real * sine], axis=0)
        spectra = three_dot(fwd_high, fwd_low, turned)
        sr, si = spectra[:tokens], spectra[tokens:]
        a_r, b_r, h_r = (sr[:, i * LANES:(i + 1) * LANES] for i in range(3))
        a_i, b_i, h_i = (si[:, i * LANES:(i + 1) * LANES] for i in range(3))
        lane = lax.broadcasted_iota(jnp.int32, h_i.shape, 1)
        h_i = jnp.where(lane < half_lanes, h_i, -h_i)
        swap = lambda v: pltpu.roll(v, half_lanes, 1)
        ga_r, ga_i, gb_r, gb_i = swap(a_r), swap(a_i), swap(b_r), swap(b_i)
        prod_r = jnp.concatenate([
            a_r * h_r - a_i * h_i,
            b_r * h_r - b_i * h_i,
            a_r * ga_r + a_i * ga_i + b_r * gb_r + b_i * gb_i], axis=1)
        prod_i = jnp.concatenate([
            a_r * h_i + a_i * h_r,
            b_r * h_i + b_i * h_r,
            a_r * ga_i - a_i * ga_r + b_r * gb_i - b_i * gb_r], axis=1)
        back = three_dot(inv_high, inv_low, jnp.concatenate([prod_r, prod_i], axis=0))
        br, bi = back[:tokens], back[tokens:]
        weight = jnp.where((k == 0) | (k == seq_count), 0.5 / (seq_count * tokens), 1.0 / (seq_count * tokens))
        cosine, sine = cosine * weight, sine * weight
        spec_ref[k, 0] = br * cosine - bi * sine
        spec_ref[k, 1] = bi * cosine + br * sine
        return carry

    lax.fori_loop(0, seq_count + 1, middle, 0)

    def synthesise(chunk, carry):
        rows = pl.ds(pl.multiple_of(chunk * 8, 8), 8)
        for signal in range(3):
            lanes = slice(signal * LANES, (signal + 1) * LANES)
            terms = [(spec_ref[k, 0, rows, lanes], spec_ref[k, 1, rows, lanes]) for k in range(seq_count + 1)]
            for n, value in enumerate(real_from_half(terms, size, True)):
                if signal < 2:
                    out_pair_ref[signal, n, rows, :] = value
                else:
                    corr_scr[n, rows, :] = value
        return carry

    lax.fori_loop(0, tokens // 8, synthesise, 0)
    corr_scale = (seq_count * tokens) ** -0.5

    def gather_corr(block, carry):
        top = corr_scr[block, :half_tokens, :]
        bottom = pltpu.roll(corr_scr[block, half_tokens:, :], half_lanes, 1)
        lane = lax.broadcasted_iota(jnp.int32, top.shape, 1)
        out_corr_ref[block] = jnp.where(lane < half_lanes, top, bottom) * corr_scale
        return carry

    lax.fori_loop(0, seq_count, gather_corr, 0)


def left_mask(shape):
    return lax.broadcasted_iota(jnp.int32, shape, 1) < LANES // 2


def gate_kernel(query_ref, key_ref, value_ref, out_ref, pair_ref):
    mixed = key_ref[...].astype(jnp.float32) * value_ref[...].astype(jnp.float32)
    gated = out_ref[...].astype(jnp.float32) * query_ref[...].astype(jnp.float32)
    left = left_mask(mixed.shape)
    pair_ref[0] = jnp.where(left, mixed, pltpu.roll(gated, LANES // 2, 1))
    pair_ref[1] = jnp.where(left, pltpu.roll(mixed, LANES // 2, 1), gated)


def finish_kernel(pair_ref, query_ref, key_ref, value_ref, out_ref, skip_ref, gq_ref, gk_ref, gv_ref):
    query_f = query_ref[...].astype(jnp.float32)
    key_f = key_ref[...].astype(jnp.float32)
    value_f = value_ref[...].astype(jnp.float32)
    out_f = out_ref[...].astype(jnp.float32)
    first, second = pair_ref[0], pair_ref[1]
    left = left_mask(first.shape)
    skip = skip_ref[...]
    conv = jnp.where(left, first, pltpu.roll(second, LANES // 2, 1)) + skip * (key_f * value_f)
    back = jnp.where(left, pltpu.roll(first, LANES // 2, 1), second) + skip * (out_f * query_f)
    gq_ref[...] = (out_f * conv).astype(jnp.bfloat16)
    gk_ref[...] = (back * value_f).astype(jnp.bfloat16)
    gv_ref[...] = (back * key_f).astype(jnp.bfloat16)


def tables(seq_count, tokens):
    index = np.arange(tokens)
    angle = 2.0 * np.pi / tokens * (index[:, None] * index[None, :] % tokens)
    cosine, sine = np.cos(angle), np.sin(angle)
    forward = np.block([[cosine, sine], [-sine, cosine]]).astype(np.float32)
    inverse = np.block([[cosine, -sine], [sine, cosine]]).astype(np.float32)

    def pieces(table):
        table = jnp.asarray(table)
        return jnp.stack(split_bf16(table))

    turn = 2.0 * np.pi / (2 * seq_count * tokens) * (np.arange(seq_count + 1)[:, None] * index[None, :])
    twiddle = np.stack([np.cos(turn), np.sin(turn)], axis=1).astype(np.float32)
    twiddle = jnp.broadcast_to(jnp.asarray(twiddle)[..., None], twiddle.shape + (LANES,))
    return pieces(forward), pieces(inverse), twiddle


def fast_shards(query_gate, key_input, value_input, grad_output, filter_raw, skip_gain):
    seq_count, ch_count = lax.axis_size("seq"), lax.axis_size("ch")
    owners = seq_count * ch_count
    _, tokens, channels = key_input.shape
    length = seq_count * tokens
    width = channels // owners
    groups = channels // LANES
    block = pl.BlockSpec((None, tokens, LANES), lambda i: (0, 0, i))
    pair_block = pl.BlockSpec((2, tokens, LANES), lambda i: (i, 0, 0))
    params = pltpu.CompilerParams(vmem_limit_bytes=VMEM_LIMIT)
    pair = pl.pallas_call(
        gate_kernel,
        grid=(groups,),
        in_specs=[block] * 4,
        out_specs=pair_block,
        out_shape=jax.ShapeDtypeStruct((owners, tokens, LANES), jnp.float32),
        name="gate",
    )(query_gate, key_input, value_input, grad_output)
    mine = lax.axis_index("ch") * (channels // ch_count)
    taps = lax.dynamic_slice_in_dim(filter_raw, mine, channels // ch_count, axis=1)
    taps = taps.astype(jnp.float32) * length ** (-0.5)
    taps = taps.reshape(2, tokens // 2, seq_count, width).transpose(2, 1, 0, 3)
    taps = taps.reshape(seq_count, tokens // 2, LANES)
    pair = lax.all_to_all(pair, ("ch", "seq"), split_axis=0, concat_axis=0, tiled=True)
    taps = lax.all_to_all(taps, "seq", split_axis=0, concat_axis=0, tiled=True)
    pair, corr = pl.pallas_call(
        lambda *refs: fft_kernel(seq_count, tokens, *refs),
        out_shape=(
            jax.ShapeDtypeStruct((ch_count, seq_count, tokens, LANES), jnp.float32),
            jax.ShapeDtypeStruct((seq_count, tokens // 2, LANES), jnp.float32),
        ),
        scratch_shapes=[
            pltpu.VMEM((seq_count + 1, 2, tokens, 3 * LANES), jnp.float32),
            pltpu.VMEM((seq_count, tokens, LANES), jnp.float32),
            pltpu.VMEM((seq_count, tokens, LANES), jnp.float32),
        ],
        compiler_params=params,
        name="convolve",
    )(pair.reshape(ch_count, seq_count, tokens, LANES), taps, *tables(seq_count, tokens))
    pair = lax.all_to_all(pair.reshape(owners, tokens, LANES), ("ch", "seq"), split_axis=0, concat_axis=0, tiled=True)
    corr = lax.all_to_all(corr, "seq", split_axis=0, concat_axis=0, tiled=True)
    grads = pl.pallas_call(
        finish_kernel,
        grid=(groups,),
        in_specs=[pair_block] + [block] * 4 + [pl.BlockSpec((1, LANES), lambda i: (0, i))],
        out_specs=[block] * 3,
        out_shape=[jax.ShapeDtypeStruct(key_input.shape, jnp.bfloat16)] * 3,
        name="finish",
    )(pair, query_gate, key_input, value_input, grad_output, skip_gain[None])
    corr = corr.reshape(seq_count, tokens // 2, 2, width).transpose(2, 1, 0, 3)
    return (*grads, corr.reshape(tokens, seq_count * width))


def solution(mesh):
    in_specs = (
        P("ch", "seq", None),
        P("ch", "seq", None),
        P("ch", "seq", None),
        P("ch", "seq", None),
        P("seq", None),
        P(),
    )
    out_specs = (P("ch", "seq", None), P("ch", "seq", None), P("ch", "seq", None), P("seq", "ch"))

    def body(*arrays):
        seq_count, ch_count = mesh.shape["seq"], mesh.shape["ch"]
        _, tokens, channels = arrays[0].shape
        fits = ch_count == 2 and tokens == LANES and channels == seq_count * LANES and seq_count <= 32
        return (fast_shards if fits else shards)(*arrays)

    return jax.shard_map(body, mesh=mesh, in_specs=in_specs, out_specs=out_specs, check_vma=False)
```

```python
import math

import numpy as np

import jax
import jax.numpy as jnp
from jax import lax
from jax.experimental import pallas as pl
from jax.experimental.pallas import tpu as pltpu
from jax.sharding import PartitionSpec as P


def angle_table(row_index, col_index, modulus):
    turn_count = row_index[:, None] * col_index[None, :] % modulus
    angles = turn_count.astype(jnp.float32) * (2.0 * math.pi / modulus)
    return (jnp.cos(angles), jnp.sin(angles))


def contract(pattern, table, operand):
    return jnp.einsum(
        pattern, table, operand, precision=lax.Precision.HIGHEST, preferred_element_type=jnp.float32
    )


def rotate(pattern, cos_table, sin_table, sense_sign, real_part, imag_part, want_imag):
    if imag_part is None:
        cos_term = contract(pattern, cos_table, real_part)
        return (cos_term, sense_sign * contract(pattern, sin_table, real_part))
    real_out = contract(pattern, cos_table, real_part) - sense_sign * contract(
        pattern, sin_table, imag_part
    )
    if not want_imag:
        return (real_out, None)
    imag_out = contract(pattern, cos_table, imag_part) + sense_sign * contract(
        pattern, sin_table, real_part
    )
    return (real_out, imag_out)


def twist(cos_table, sin_table, sense_sign, real_part, imag_part):
    return (
        real_part * cos_table - sense_sign * imag_part * sin_table,
        imag_part * cos_table + sense_sign * real_part * sin_table,
    )


def spectral_terms(z_real, z_imag, g_real, g_imag, h_real, h_imag):
    conv_real = z_real * h_real - z_imag * h_imag
    conv_imag = z_real * h_imag + z_imag * h_real
    back_real = h_real * g_real + h_imag * g_imag
    back_imag = h_real * g_imag - h_imag * g_real
    corr_real = z_real * g_real + z_imag * g_imag
    corr_imag = z_real * g_imag - z_imag * g_real
    return (conv_real - back_imag, conv_imag + back_real, corr_real, corr_imag)


def shards(query_gate, key_input, value_input, grad_output, filter_raw, skip_gain):
    seq_count = lax.axis_size("seq")
    key_f = key_input[0].astype(jnp.float32)
    value_f = value_input[0].astype(jnp.float32)
    out_f = grad_output[0].astype(jnp.float32)
    mixed = key_f * value_f
    gated = out_f * query_gate[0].astype(jnp.float32)
    tokens, channels = mixed.shape
    seq_length = tokens * seq_count
    full_length = 2 * seq_length
    inverse_scale = 1.0 / full_length
    filter_taps = filter_raw.astype(jnp.float32) * seq_length ** (-0.5)
    freq_one = jnp.arange(2 * seq_count, dtype=jnp.int32)
    block_index = jnp.arange(seq_count, dtype=jnp.int32)
    offset_index = jnp.arange(tokens, dtype=jnp.int32)
    cos_one, sin_one = angle_table(freq_one, block_index, 2 * seq_count)
    cos_inv, sin_inv = angle_table(block_index, freq_one, 2 * seq_count)
    cos_two, sin_two = angle_table(offset_index, offset_index, tokens)
    local_width = channels // seq_count
    arrived = (
        lax.all_to_all(mixed.T, "seq", split_axis=0, concat_axis=1, tiled=True),
        lax.all_to_all(gated.T, "seq", split_axis=0, concat_axis=1, tiled=True),
        lax.all_to_all(filter_taps.T, "seq", split_axis=0, concat_axis=1, tiled=True),
    )
    cos_tw, sin_tw = angle_table(freq_one, offset_index, full_length)
    spectra = []
    for line_data in arrived:
        lines = line_data.reshape(local_width, seq_count, tokens)
        real_part, imag_part = rotate("kn,cnm->ckm", cos_one, sin_one, -1.0, lines, None, True)
        real_part, imag_part = twist(cos_tw, sin_tw, -1.0, real_part, imag_part)
        spectra.append(rotate("jm,ckm->ckj", cos_two, sin_two, -1.0, real_part, imag_part, True))
    packed_real, packed_imag, corr_real, corr_imag = spectral_terms(
        spectra[0][0], spectra[0][1], spectra[1][0], spectra[1][1], spectra[2][0], spectra[2][1]
    )
    pr_mid, pi_mid = rotate("mj,ckj->ckm", cos_two, sin_two, 1.0, packed_real, packed_imag, True)
    pr_mid, pi_mid = twist(cos_tw, sin_tw, 1.0, pr_mid, pi_mid)
    cr_mid, ci_mid = rotate("mj,ckj->ckm", cos_two, sin_two, 1.0, corr_real, corr_imag, True)
    cr_mid, ci_mid = twist(cos_tw, sin_tw, 1.0, cr_mid, ci_mid)
    conv_lines, back_lines = rotate("nk,ckm->cnm", cos_inv, sin_inv, 1.0, pr_mid, pi_mid, True)
    corr_lines = rotate("nk,ckm->cnm", cos_inv, sin_inv, 1.0, cr_mid, ci_mid, False)[0]
    conv_lines = (conv_lines * inverse_scale).reshape(local_width, seq_length)
    back_lines = (back_lines * inverse_scale).reshape(local_width, seq_length)
    corr_lines = (corr_lines * inverse_scale).reshape(local_width, seq_length)
    returned = (
        lax.all_to_all(conv_lines, "seq", split_axis=1, concat_axis=0, tiled=True),
        lax.all_to_all(back_lines, "seq", split_axis=1, concat_axis=0, tiled=True),
        lax.all_to_all(corr_lines, "seq", split_axis=1, concat_axis=0, tiled=True),
    )
    conv_time = returned[0].T
    back_time = returned[1].T
    corr_time = returned[2].T
    conv_full = conv_time + skip_gain * mixed
    back_full = back_time + skip_gain * gated
    grad_query = (out_f * conv_full).astype(jnp.bfloat16)[None]
    grad_key = (back_full * value_f).astype(jnp.bfloat16)[None]
    grad_value = (back_full * key_f).astype(jnp.bfloat16)[None]
    grad_filter = lax.psum_scatter(
        corr_time * seq_length ** (-0.5), "ch", scatter_dimension=1, tiled=True
    )
    return (grad_query, grad_key, grad_value, grad_filter)


LANES = 128
VMEM_LIMIT = 60 * 1024 * 1024


def times_root(pair, turn, size):
    real, imag = pair
    turn %= size
    if turn == 0:
        return pair
    if 4 * turn == size:
        return (-imag, real)
    if 2 * turn == size:
        return (-real, -imag)
    if 4 * turn == 3 * size:
        return (imag, -real)
    cosine = math.cos(2.0 * math.pi * turn / size)
    sine = math.sin(2.0 * math.pi * turn / size)
    return (real * cosine - imag * sine, real * sine + imag * cosine)


def complex_dft(values, sense):
    size = len(values)
    if size == 1:
        return values
    even = complex_dft(values[0::2], sense)
    odd = complex_dft(values[1::2], sense)
    low, high = [], []
    for k in range(size // 2):
        er, ei = even[k]
        tr, ti = times_root(odd[k], sense * k, size)
        low.append((er + tr, ei + ti))
        high.append((er - tr, ei - ti))
    return low + high


def half_spectrum(values, size):
    if size == 2:
        return [(values[0] + values[1], None), (values[0] - values[1], None)]
    half, quarter = size // 2, size // 4
    if len(values) == half:
        total, difference = values, values
    else:
        total = [values[n] + values[n + half] for n in range(half)]
        difference = [values[n] - values[n + half] for n in range(half)]
    out = [None] * (half + 1)
    out[0::2] = half_spectrum(total, half)
    turned = [times_root((difference[n], -difference[n + quarter]), -n, size) for n in range(quarter)]
    for index, (real, imag) in enumerate(complex_dft(turned, -1)):
        k = 1 + 4 * index
        if k <= half:
            out[k] = (real, imag)
        else:
            out[size - k] = (real, -imag)
    return out


def real_from_half(terms, size, first_half):
    if size == 2:
        return [terms[0][0] + terms[1][0], terms[0][0] - terms[1][0]]
    half, quarter = size // 2, size // 4
    even = real_from_half(terms[0::2], half, False)
    chosen = []
    for index in range(quarter):
        k = 1 + 4 * index
        if k <= half:
            chosen.append(terms[k])
        else:
            real, imag = terms[size - k]
            chosen.append((real, -imag))
    turned = [times_root(pair, n, size) for n, pair in enumerate(complex_dft(chosen, 1))]
    odd = [pair[0] for pair in turned] + [-pair[1] for pair in turned]
    out = [even[n] + odd[n] for n in range(half)]
    if first_half:
        return out
    return out + [even[n] - odd[n] for n in range(half)]


def split_bf16(value):
    high = value.astype(jnp.bfloat16)
    return high, (value - high.astype(jnp.float32)).astype(jnp.bfloat16)


def three_dot(table_high, table_low, value):
    high, low = split_bf16(value)
    dot = lambda a, b: jnp.dot(a, b, preferred_element_type=jnp.float32)
    return dot(table_high, high) + (dot(table_high, low) + dot(table_low, high))


def fft_kernel(seq_count, tokens, pair_ref, fwd_ref, inv_ref, tw_ref, out_pair_ref, out_corr_ref, spec_ref, taps_scr, corr_scr):
    half_lanes = LANES // 2
    half_tokens = tokens // 2
    size = 2 * seq_count

    def spread_taps(block, carry):
        for part in range(2):
            packed = pair_ref[part, block, tokens:, :]
            rolled = pltpu.roll(packed, half_lanes, 1)
            left = left_mask(packed.shape)
            start, quarter = part * half_tokens, half_tokens // 2
            taps_scr[block, start:start + quarter, :] = jnp.where(left, packed, rolled)
            taps_scr[block, start + quarter:start + half_tokens, :] = jnp.where(left, rolled, packed)
        return carry

    lax.fori_loop(0, seq_count, spread_taps, 0)

    def analyse(chunk, carry):
        rows = pl.ds(pl.multiple_of(chunk * 8, 8), 8)
        for signal in range(3):
            lanes = slice(signal * LANES, (signal + 1) * LANES)
            if signal < 2:
                values = [pair_ref[signal, n, rows, :] for n in range(seq_count)]
            else:
                values = [taps_scr[n, rows, :] for n in range(seq_count)]
            for k, (real, imag) in enumerate(half_spectrum(values, size)):
                spec_ref[k, 0, rows, lanes] = real
                spec_ref[k, 1, rows, lanes] = jnp.zeros_like(real) if imag is None else imag
        return carry

    lax.fori_loop(0, tokens // 8, analyse, 0)

    fwd_high, fwd_low = fwd_ref[0], fwd_ref[1]
    inv_high, inv_low = inv_ref[0], inv_ref[1]

    def middle(k, carry):
        cosine = jnp.concatenate([tw_ref[k, 0]] * 3, axis=1)
        sine = jnp.concatenate([tw_ref[k, 1]] * 3, axis=1)
        real, imag = spec_ref[k, 0], spec_ref[k, 1]
        turned = jnp.concatenate([real * cosine + imag * sine, imag * cosine - real * sine], axis=0)
        spectra = three_dot(fwd_high, fwd_low, turned)
        sr, si = spectra[:tokens], spectra[tokens:]
        a_r, b_r, h_r = (sr[:, i * LANES:(i + 1) * LANES] for i in range(3))
        a_i, b_i, h_i = (si[:, i * LANES:(i + 1) * LANES] for i in range(3))
        lane = lax.broadcasted_iota(jnp.int32, h_i.shape, 1)
        h_i = jnp.where(lane < half_lanes, h_i, -h_i)
        swap = lambda v: pltpu.roll(v, half_lanes, 1)
        ga_r, ga_i, gb_r, gb_i = swap(a_r), swap(a_i), swap(b_r), swap(b_i)
        prod_r = jnp.concatenate([
            a_r * h_r - a_i * h_i,
            b_r * h_r - b_i * h_i,
            a_r * ga_r + a_i * ga_i + b_r * gb_r + b_i * gb_i], axis=1)
        prod_i = jnp.concatenate([
            a_r * h_i + a_i * h_r,
            b_r * h_i + b_i * h_r,
            a_r * ga_i - a_i * ga_r + b_r * gb_i - b_i * gb_r], axis=1)
        back = three_dot(inv_high, inv_low, jnp.concatenate([prod_r, prod_i], axis=0))
        br, bi = back[:tokens], back[tokens:]
        weight = jnp.where((k == 0) | (k == seq_count), 0.5 / (seq_count * tokens), 1.0 / (seq_count * tokens))
        cosine, sine = cosine * weight, sine * weight
        spec_ref[k, 0] = br * cosine - bi * sine
        spec_ref[k, 1] = bi * cosine + br * sine
        return carry

    lax.fori_loop(0, seq_count + 1, middle, 0)

    def synthesise(chunk, carry):
        rows = pl.ds(pl.multiple_of(chunk * 8, 8), 8)
        for signal in range(3):
            lanes = slice(signal * LANES, (signal + 1) * LANES)
            terms = [(spec_ref[k, 0, rows, lanes], spec_ref[k, 1, rows, lanes]) for k in range(seq_count + 1)]
            for n, value in enumerate(real_from_half(terms, size, True)):
                if signal < 2:
                    out_pair_ref[signal, n, rows, :] = value
                else:
                    corr_scr[n, rows, :] = value
        return carry

    lax.fori_loop(0, tokens // 8, synthesise, 0)
    corr_scale = (seq_count * tokens) ** -0.5

    def gather_corr(block, carry):
        top = corr_scr[block, :half_tokens, :]
        bottom = pltpu.roll(corr_scr[block, half_tokens:, :], half_lanes, 1)
        lane = lax.broadcasted_iota(jnp.int32, top.shape, 1)
        out_corr_ref[block] = jnp.where(lane < half_lanes, top, bottom) * corr_scale
        return carry

    lax.fori_loop(0, seq_count, gather_corr, 0)


def left_mask(shape):
    return lax.broadcasted_iota(jnp.int32, shape, 1) < LANES // 2


def far_first(seq_count, ch_count):
    steps = sorted(range(seq_count), key=lambda step: abs(2 * step - seq_count))
    return [(step, turn) for step in steps for turn in range(ch_count) if step or turn]


def greet(seq_count, ch_count, me_seq, me_ch):
    barrier = pltpu.get_barrier_semaphore()
    partners = far_first(seq_count, ch_count)
    for step, turn in partners:
        pl.semaphore_signal(barrier, inc=1, device_id=partner_of(step, turn, seq_count, ch_count, me_seq, me_ch), device_id_type=pl.DeviceIdType.MESH)
    pl.semaphore_wait(barrier, len(partners))


def partner_of(step, turn, seq_count, ch_count, me_seq, me_ch):
    return {"seq": lax.rem(me_seq + step, seq_count), "ch": lax.rem(me_ch + turn, ch_count)}


def exchange(sends, seq_count, ch_count, me_seq, me_ch):
    copies = []
    for step, turn in far_first(seq_count, ch_count):
        partner = partner_of(step, turn, seq_count, ch_count, me_seq, me_ch)
        for source, target, send_sem, recv_sem, same_ch in sends:
            if same_ch and turn:
                continue
            if same_ch:
                give, take, slot = partner["seq"], me_seq, step
            else:
                give, take, slot = partner["ch"] * seq_count + partner["seq"], me_ch * seq_count + me_seq, step * ch_count + turn
            copy = pltpu.make_async_remote_copy(
                src_ref=source.at[give],
                dst_ref=target.at[take],
                send_sem=send_sem.at[slot],
                recv_sem=recv_sem.at[slot],
                device_id=partner,
                device_id_type=pl.DeviceIdType.MESH,
            )
            copy.start()
            copies.append(copy)
    return copies


def gate_kernel(seq_count, ch_count, query_ref, key_ref, value_ref, out_ref, filter_ref, pair_ref, send, recv, send_sem, recv_sem):
    me_seq, me_ch = lax.axis_index("seq"), lax.axis_index("ch")
    tokens = key_ref.shape[0]
    share = tokens // ch_count
    scale = (seq_count * tokens) ** -0.5
    half_lanes = LANES // 2

    def prepare(group, carry):
        lanes = pl.ds(pl.multiple_of(group * LANES, LANES), LANES)
        mixed = key_ref[:, lanes].astype(jnp.float32) * value_ref[:, lanes].astype(jnp.float32)
        gated = out_ref[:, lanes].astype(jnp.float32) * query_ref[:, lanes].astype(jnp.float32)
        left = left_mask(mixed.shape)
        send[2 * group, :tokens, :] = jnp.where(left, mixed, pltpu.roll(gated, half_lanes, 1))
        send[2 * group + 1, :tokens, :] = jnp.where(left, pltpu.roll(mixed, half_lanes, 1), gated)
        rows = pl.ds(pl.multiple_of(me_ch * share, share), share)
        taps = filter_ref[rows, lanes].astype(jnp.float32) * scale
        top, bottom = taps[:share // 2], taps[share // 2:]
        left = left_mask(top.shape)
        send[2 * group, tokens:, :] = jnp.where(left, top, pltpu.roll(bottom, half_lanes, 1))
        send[2 * group + 1, tokens:, :] = jnp.where(left, pltpu.roll(top, half_lanes, 1), bottom)
        return carry

    lax.fori_loop(0, seq_count, prepare, 0)
    greet(seq_count, ch_count, me_seq, me_ch)
    copies = exchange([(send, recv, send_sem, recv_sem, False)], seq_count, ch_count, me_seq, me_ch)
    mine = me_ch * seq_count + me_seq
    recv[mine] = send[mine]
    for copy in copies:
        copy.wait()

    def hand_over(owner, carry):
        pair_ref[owner] = recv[owner]
        return carry

    lax.fori_loop(0, seq_count * ch_count, hand_over, 0)


def left_mask(shape):
    return lax.broadcasted_iota(jnp.int32, shape, 1) < LANES // 2


def finish_kernel(seq_count, ch_count, pair_ref, corr_ref, query_ref, key_ref, value_ref, out_ref, skip_ref, gq_ref, gk_ref, gv_ref, gf_ref, recv, corr_recv, send_sem, recv_sem, corr_send_sem, corr_recv_sem):
    me_seq, me_ch = lax.axis_index("seq"), lax.axis_index("ch")
    half_lanes = LANES // 2
    half_tokens = key_ref.shape[0] // 2
    greet(seq_count, ch_count, me_seq, me_ch)
    copies = exchange(
        [(pair_ref, recv, send_sem, recv_sem, False), (corr_ref, corr_recv, corr_send_sem, corr_recv_sem, True)],
        seq_count, ch_count, me_seq, me_ch)
    mine = me_ch * seq_count + me_seq
    recv[mine] = pair_ref[mine]
    corr_recv[me_seq] = corr_ref[me_seq]
    for copy in copies:
        copy.wait()

    def finish(group, carry):
        lanes = pl.ds(pl.multiple_of(group * LANES, LANES), LANES)
        query_f = query_ref[:, lanes].astype(jnp.float32)
        key_f = key_ref[:, lanes].astype(jnp.float32)
        value_f = value_ref[:, lanes].astype(jnp.float32)
        out_f = out_ref[:, lanes].astype(jnp.float32)
        first, second = recv[2 * group], recv[2 * group + 1]
        left = left_mask(first.shape)
        skip = skip_ref[:, lanes]
        conv = jnp.where(left, first, pltpu.roll(second, half_lanes, 1)) + skip * (key_f * value_f)
        back = jnp.where(left, pltpu.roll(first, half_lanes, 1), second) + skip * (out_f * query_f)
        gq_ref[:, lanes] = (out_f * conv).astype(jnp.bfloat16)
        gk_ref[:, lanes] = (back * value_f).astype(jnp.bfloat16)
        gv_ref[:, lanes] = (back * key_f).astype(jnp.bfloat16)
        return carry

    lax.fori_loop(0, seq_count, finish, 0)

    def finish_corr(group, carry):
        lanes = pl.ds(pl.multiple_of(group * LANES, LANES), LANES)
        first, second = corr_recv[2 * group], corr_recv[2 * group + 1]
        left = left_mask(first.shape)
        gf_ref[:half_tokens, lanes] = jnp.where(left, first, pltpu.roll(second, half_lanes, 1))
        gf_ref[half_tokens:, lanes] = jnp.where(left, pltpu.roll(first, half_lanes, 1), second)
        return carry

    lax.fori_loop(0, seq_count // 2, finish_corr, 0)


def tables(seq_count, tokens):
    index = np.arange(tokens)
    angle = 2.0 * np.pi / tokens * (index[:, None] * index[None, :] % tokens)
    cosine, sine = np.cos(angle), np.sin(angle)
    forward = np.block([[cosine, sine], [-sine, cosine]]).astype(np.float32)
    inverse = np.block([[cosine, -sine], [sine, cosine]]).astype(np.float32)

    def pieces(table):
        table = jnp.asarray(table)
        return jnp.stack(split_bf16(table))

    turn = 2.0 * np.pi / (2 * seq_count * tokens) * (np.arange(seq_count + 1)[:, None] * index[None, :])
    twiddle = np.stack([np.cos(turn), np.sin(turn)], axis=1).astype(np.float32)
    twiddle = jnp.broadcast_to(jnp.asarray(twiddle)[..., None], twiddle.shape + (LANES,))
    return pieces(forward), pieces(inverse), twiddle


def fast_shards(query_gate, key_input, value_input, grad_output, filter_raw, skip_gain):
    seq_count, ch_count = lax.axis_size("seq"), lax.axis_size("ch")
    owners = seq_count * ch_count
    _, tokens, channels = key_input.shape
    rows = tokens + tokens // (2 * ch_count)
    vmem = pl.BlockSpec(memory_space=pltpu.VMEM)
    signals = (query_gate[0], key_input[0], value_input[0], grad_output[0])
    pair = pl.pallas_call(
        lambda *refs: gate_kernel(seq_count, ch_count, *refs),
        in_specs=[vmem] * 5,
        out_specs=vmem,
        out_shape=jax.ShapeDtypeStruct((owners, rows, LANES), jnp.float32),
        scratch_shapes=[
            pltpu.VMEM((owners, rows, LANES), jnp.float32),
            pltpu.VMEM((owners, rows, LANES), jnp.float32),
            pltpu.SemaphoreType.DMA((owners,)),
            pltpu.SemaphoreType.DMA((owners,)),
        ],
        compiler_params=pltpu.CompilerParams(vmem_limit_bytes=VMEM_LIMIT, collective_id=0, has_side_effects=True),
        name="gate",
    )(*signals, filter_raw)
    pair, corr = pl.pallas_call(
        lambda *refs: fft_kernel(seq_count, tokens, *refs),
        out_shape=(
            jax.ShapeDtypeStruct((ch_count, seq_count, tokens, LANES), jnp.float32),
            jax.ShapeDtypeStruct((seq_count, tokens // 2, LANES), jnp.float32),
        ),
        scratch_shapes=[
            pltpu.VMEM((seq_count + 1, 2, tokens, 3 * LANES), jnp.float32),
            pltpu.VMEM((seq_count, tokens, LANES), jnp.float32),
            pltpu.VMEM((seq_count, tokens, LANES), jnp.float32),
        ],
        compiler_params=pltpu.CompilerParams(vmem_limit_bytes=VMEM_LIMIT),
        name="convolve",
    )(pair.reshape(ch_count, seq_count, rows, LANES), *tables(seq_count, tokens))
    grads = pl.pallas_call(
        lambda *refs: finish_kernel(seq_count, ch_count, *refs),
        in_specs=[vmem] * 7,
        out_specs=[vmem] * 4,
        out_shape=[jax.ShapeDtypeStruct((tokens, channels), jnp.bfloat16)] * 3
        + [jax.ShapeDtypeStruct((tokens, channels // ch_count), jnp.float32)],
        scratch_shapes=[
            pltpu.VMEM((owners, tokens, LANES), jnp.float32),
            pltpu.VMEM((seq_count, tokens // 2, LANES), jnp.float32),
            pltpu.SemaphoreType.DMA((owners,)),
            pltpu.SemaphoreType.DMA((owners,)),
            pltpu.SemaphoreType.DMA((seq_count,)),
            pltpu.SemaphoreType.DMA((seq_count,)),
        ],
        compiler_params=pltpu.CompilerParams(vmem_limit_bytes=VMEM_LIMIT, collective_id=1, has_side_effects=True),
        name="finish",
    )(pair.reshape(owners, tokens, LANES), corr, *signals, skip_gain[None])
    return (grads[0][None], grads[1][None], grads[2][None], grads[3])


def solution(mesh):
    in_specs = (
        P("ch", "seq", None),
        P("ch", "seq", None),
        P("ch", "seq", None),
        P("ch", "seq", None),
        P("seq", None),
        P(),
    )
    out_specs = (P("ch", "seq", None), P("ch", "seq", None), P("ch", "seq", None), P("seq", "ch"))

    def body(*arrays):
        seq_count, ch_count = mesh.shape["seq"], mesh.shape["ch"]
        _, tokens, channels = arrays[0].shape
        fits = ch_count == 2 and tokens == LANES and channels == seq_count * LANES and seq_count <= 32
        return (fast_shards if fits else shards)(*arrays)

    return jax.shard_map(body, mesh=mesh, in_specs=in_specs, out_specs=out_specs, check_vma=False)
```

```python
import math

import numpy as np

import jax
import jax.numpy as jnp
from jax import lax
from jax.experimental import pallas as pl
from jax.experimental.pallas import tpu as pltpu
from jax.sharding import PartitionSpec as P


def angle_table(row_index, col_index, modulus):
    turn_count = row_index[:, None] * col_index[None, :] % modulus
    angles = turn_count.astype(jnp.float32) * (2.0 * math.pi / modulus)
    return (jnp.cos(angles), jnp.sin(angles))


def contract(pattern, table, operand):
    return jnp.einsum(
        pattern, table, operand, precision=lax.Precision.HIGHEST, preferred_element_type=jnp.float32
    )


def rotate(pattern, cos_table, sin_table, sense_sign, real_part, imag_part, want_imag):
    if imag_part is None:
        cos_term = contract(pattern, cos_table, real_part)
        return (cos_term, sense_sign * contract(pattern, sin_table, real_part))
    real_out = contract(pattern, cos_table, real_part) - sense_sign * contract(
        pattern, sin_table, imag_part
    )
    if not want_imag:
        return (real_out, None)
    imag_out = contract(pattern, cos_table, imag_part) + sense_sign * contract(
        pattern, sin_table, real_part
    )
    return (real_out, imag_out)


def twist(cos_table, sin_table, sense_sign, real_part, imag_part):
    return (
        real_part * cos_table - sense_sign * imag_part * sin_table,
        imag_part * cos_table + sense_sign * real_part * sin_table,
    )


def spectral_terms(z_real, z_imag, g_real, g_imag, h_real, h_imag):
    conv_real = z_real * h_real - z_imag * h_imag
    conv_imag = z_real * h_imag + z_imag * h_real
    back_real = h_real * g_real + h_imag * g_imag
    back_imag = h_real * g_imag - h_imag * g_real
    corr_real = z_real * g_real + z_imag * g_imag
    corr_imag = z_real * g_imag - z_imag * g_real
    return (conv_real - back_imag, conv_imag + back_real, corr_real, corr_imag)


def shards(query_gate, key_input, value_input, grad_output, filter_raw, skip_gain):
    seq_count = lax.axis_size("seq")
    key_f = key_input[0].astype(jnp.float32)
    value_f = value_input[0].astype(jnp.float32)
    out_f = grad_output[0].astype(jnp.float32)
    mixed = key_f * value_f
    gated = out_f * query_gate[0].astype(jnp.float32)
    tokens, channels = mixed.shape
    seq_length = tokens * seq_count
    full_length = 2 * seq_length
    inverse_scale = 1.0 / full_length
    filter_taps = filter_raw.astype(jnp.float32) * seq_length ** (-0.5)
    freq_one = jnp.arange(2 * seq_count, dtype=jnp.int32)
    block_index = jnp.arange(seq_count, dtype=jnp.int32)
    offset_index = jnp.arange(tokens, dtype=jnp.int32)
    cos_one, sin_one = angle_table(freq_one, block_index, 2 * seq_count)
    cos_inv, sin_inv = angle_table(block_index, freq_one, 2 * seq_count)
    cos_two, sin_two = angle_table(offset_index, offset_index, tokens)
    local_width = channels // seq_count
    arrived = (
        lax.all_to_all(mixed.T, "seq", split_axis=0, concat_axis=1, tiled=True),
        lax.all_to_all(gated.T, "seq", split_axis=0, concat_axis=1, tiled=True),
        lax.all_to_all(filter_taps.T, "seq", split_axis=0, concat_axis=1, tiled=True),
    )
    cos_tw, sin_tw = angle_table(freq_one, offset_index, full_length)
    spectra = []
    for line_data in arrived:
        lines = line_data.reshape(local_width, seq_count, tokens)
        real_part, imag_part = rotate("kn,cnm->ckm", cos_one, sin_one, -1.0, lines, None, True)
        real_part, imag_part = twist(cos_tw, sin_tw, -1.0, real_part, imag_part)
        spectra.append(rotate("jm,ckm->ckj", cos_two, sin_two, -1.0, real_part, imag_part, True))
    packed_real, packed_imag, corr_real, corr_imag = spectral_terms(
        spectra[0][0], spectra[0][1], spectra[1][0], spectra[1][1], spectra[2][0], spectra[2][1]
    )
    pr_mid, pi_mid = rotate("mj,ckj->ckm", cos_two, sin_two, 1.0, packed_real, packed_imag, True)
    pr_mid, pi_mid = twist(cos_tw, sin_tw, 1.0, pr_mid, pi_mid)
    cr_mid, ci_mid = rotate("mj,ckj->ckm", cos_two, sin_two, 1.0, corr_real, corr_imag, True)
    cr_mid, ci_mid = twist(cos_tw, sin_tw, 1.0, cr_mid, ci_mid)
    conv_lines, back_lines = rotate("nk,ckm->cnm", cos_inv, sin_inv, 1.0, pr_mid, pi_mid, True)
    corr_lines = rotate("nk,ckm->cnm", cos_inv, sin_inv, 1.0, cr_mid, ci_mid, False)[0]
    conv_lines = (conv_lines * inverse_scale).reshape(local_width, seq_length)
    back_lines = (back_lines * inverse_scale).reshape(local_width, seq_length)
    corr_lines = (corr_lines * inverse_scale).reshape(local_width, seq_length)
    returned = (
        lax.all_to_all(conv_lines, "seq", split_axis=1, concat_axis=0, tiled=True),
        lax.all_to_all(back_lines, "seq", split_axis=1, concat_axis=0, tiled=True),
        lax.all_to_all(corr_lines, "seq", split_axis=1, concat_axis=0, tiled=True),
    )
    conv_time = returned[0].T
    back_time = returned[1].T
    corr_time = returned[2].T
    conv_full = conv_time + skip_gain * mixed
    back_full = back_time + skip_gain * gated
    grad_query = (out_f * conv_full).astype(jnp.bfloat16)[None]
    grad_key = (back_full * value_f).astype(jnp.bfloat16)[None]
    grad_value = (back_full * key_f).astype(jnp.bfloat16)[None]
    grad_filter = lax.psum_scatter(
        corr_time * seq_length ** (-0.5), "ch", scatter_dimension=1, tiled=True
    )
    return (grad_query, grad_key, grad_value, grad_filter)


LANES = 128
VMEM_LIMIT = 60 * 1024 * 1024


def times_root(pair, turn, size):
    real, imag = pair
    turn %= size
    if turn == 0:
        return pair
    if 4 * turn == size:
        return (-imag, real)
    if 2 * turn == size:
        return (-real, -imag)
    if 4 * turn == 3 * size:
        return (imag, -real)
    cosine = math.cos(2.0 * math.pi * turn / size)
    sine = math.sin(2.0 * math.pi * turn / size)
    return (real * cosine - imag * sine, real * sine + imag * cosine)


def complex_dft(values, sense):
    size = len(values)
    if size == 1:
        return values
    even = complex_dft(values[0::2], sense)
    odd = complex_dft(values[1::2], sense)
    low, high = [], []
    for k in range(size // 2):
        er, ei = even[k]
        tr, ti = times_root(odd[k], sense * k, size)
        low.append((er + tr, ei + ti))
        high.append((er - tr, ei - ti))
    return low + high


def half_spectrum(values, size):
    if size == 2:
        return [(values[0] + values[1], None), (values[0] - values[1], None)]
    half, quarter = size // 2, size // 4
    if len(values) == half:
        total, difference = values, values
    else:
        total = [values[n] + values[n + half] for n in range(half)]
        difference = [values[n] - values[n + half] for n in range(half)]
    out = [None] * (half + 1)
    out[0::2] = half_spectrum(total, half)
    turned = [times_root((difference[n], -difference[n + quarter]), -n, size) for n in range(quarter)]
    for index, (real, imag) in enumerate(complex_dft(turned, -1)):
        k = 1 + 4 * index
        if k <= half:
            out[k] = (real, imag)
        else:
            out[size - k] = (real, -imag)
    return out


def real_from_half(terms, size, first_half):
    if size == 2:
        return [terms[0][0] + terms[1][0], terms[0][0] - terms[1][0]]
    half, quarter = size // 2, size // 4
    even = real_from_half(terms[0::2], half, False)
    chosen = []
    for index in range(quarter):
        k = 1 + 4 * index
        if k <= half:
            chosen.append(terms[k])
        else:
            real, imag = terms[size - k]
            chosen.append((real, -imag))
    turned = [times_root(pair, n, size) for n, pair in enumerate(complex_dft(chosen, 1))]
    odd = [pair[0] for pair in turned] + [-pair[1] for pair in turned]
    out = [even[n] + odd[n] for n in range(half)]
    if first_half:
        return out
    return out + [even[n] - odd[n] for n in range(half)]


def split_bf16(value):
    high = value.astype(jnp.bfloat16)
    return high, (value - high.astype(jnp.float32)).astype(jnp.bfloat16)


def three_dot(table_high, table_low, value):
    high, low = split_bf16(value)
    dot = lambda a, b: jnp.dot(a, b, preferred_element_type=jnp.float32)
    return dot(table_high, high) + (dot(table_high, low) + dot(table_low, high))


def far_first(seq_count, ch_count):
    steps = sorted(range(seq_count), key=lambda step: abs(2 * step - seq_count))
    return [(step, turn) for step in steps for turn in range(ch_count) if step or turn]


def partner_of(step, turn, seq_count, ch_count, me_seq, me_ch):
    return {"seq": lax.rem(me_seq + step, seq_count), "ch": lax.rem(me_ch + turn, ch_count)}


def left_mask(shape):
    return lax.broadcasted_iota(jnp.int32, shape, 1) < LANES // 2


def swap_halves(value):
    return pltpu.roll(value, LANES // 2, 1)


def greet_all(seq_count, ch_count, me_seq, me_ch):
    barrier = pltpu.get_barrier_semaphore()
    for step, turn in far_first(seq_count, ch_count):
        pl.semaphore_signal(barrier, inc=1, device_id=partner_of(step, turn, seq_count, ch_count, me_seq, me_ch), device_id_type=pl.DeviceIdType.MESH)
    return barrier


def exchange(sends, turn, seq_count, ch_count, me_seq, me_ch):
    copies = []
    for step, at in far_first(seq_count, ch_count):
        if at != turn:
            continue
        partner = partner_of(step, turn, seq_count, ch_count, me_seq, me_ch)
        for source, target, send_sem, recv_sem, per_seq in sends:
            if per_seq:
                give, take, slot = partner["seq"], me_seq, step
            else:
                give, take, slot = partner["ch"] * seq_count + partner["seq"], me_ch * seq_count + me_seq, step * ch_count + turn
            copy = pltpu.make_async_remote_copy(
                src_ref=source.at[give],
                dst_ref=target.at[take],
                send_sem=send_sem.at[slot],
                recv_sem=recv_sem.at[slot],
                device_id=partner,
                device_id_type=pl.DeviceIdType.MESH,
            )
            copy.start()
            copies.append(copy)
    return copies


def layer_kernel(
    seq_count, ch_count,
    query_ref, key_ref, value_ref, out_ref, filter_ref, skip_ref, fwd_ref, inv_ref, tw_ref,
    gq_ref, gk_ref, gv_ref, gf_ref,
    send, taps_send, recv, taps_recv, result, corr_result, back_recv, corr_recv,
    spec, taps_spec, corr_spec, taps_scr, corr_scr, tw_scr,
    send_sem, recv_sem, taps_send_sem, taps_recv_sem, back_send_sem, back_recv_sem, corr_send_sem, corr_recv_sem,
):
    me_seq, me_ch = lax.axis_index("seq"), lax.axis_index("ch")
    where_am_i = (seq_count, ch_count, me_seq, me_ch)
    tokens, channels = key_ref.shape
    half_tokens = tokens // 2
    size = 2 * seq_count
    scale = (seq_count * tokens) ** -0.5
    own = me_ch * (channels // ch_count)
    mine = me_ch * seq_count + me_seq
    barrier = greet_all(*where_am_i)

    def prepare_taps(group, carry):
        lanes = pl.ds(pl.multiple_of(own + group * LANES, LANES), LANES)
        taps = filter_ref[:, lanes].astype(jnp.float32) * scale
        top, bottom = taps[:half_tokens], taps[half_tokens:]
        left = left_mask(top.shape)
        taps_send[2 * group] = jnp.where(left, top, swap_halves(bottom))
        taps_send[2 * group + 1] = jnp.where(left, swap_halves(top), bottom)
        return carry

    lax.fori_loop(0, seq_count // 2, prepare_taps, 0)

    def prepare(group, carry):
        lanes = pl.ds(pl.multiple_of(group * LANES, LANES), LANES)
        mixed = key_ref[:, lanes].astype(jnp.float32) * value_ref[:, lanes].astype(jnp.float32)
        gated = out_ref[:, lanes].astype(jnp.float32) * query_ref[:, lanes].astype(jnp.float32)
        left = left_mask(mixed.shape)
        send[2 * group] = jnp.where(left, mixed, swap_halves(gated))
        send[2 * group + 1] = jnp.where(left, swap_halves(mixed), gated)
        return carry

    lax.fori_loop(0, seq_count, prepare, 0)
    pl.semaphore_wait(barrier, len(far_first(seq_count, ch_count)))
    arriving = [exchange([(taps_send, taps_recv, taps_send_sem, taps_recv_sem, True), (send, recv, send_sem, recv_sem, False)], 0, *where_am_i)]
    arriving.append(exchange([(send, recv, send_sem, recv_sem, False)], 1, *where_am_i))
    recv[mine] = send[mine]
    taps_recv[me_seq] = taps_send[me_seq]
    for k in range(seq_count + 1):
        for part in range(2):
            tw_scr[k, part] = jnp.broadcast_to(tw_ref[part, :, k:k + 1], (tokens, LANES))
    for copy in arriving[0]:
        copy.wait_recv()

    def spread_taps(block, carry):
        packed = taps_recv[block]
        rolled = swap_halves(packed)
        left = left_mask(packed.shape)
        taps_scr[block, :half_tokens, :] = jnp.where(left, packed, rolled)
        taps_scr[block, half_tokens:, :] = jnp.where(left, rolled, packed)
        return carry

    lax.fori_loop(0, seq_count, spread_taps, 0)

    def analyse(load, target):
        def body(chunk, carry):
            rows = pl.ds(pl.multiple_of(chunk * 8, 8), 8)
            for k, (real, imag) in enumerate(half_spectrum([load(n, rows) for n in range(seq_count)], size)):
                target[k, 0, rows, :] = real
                target[k, 1, rows, :] = jnp.zeros_like(real) if imag is None else imag
            return carry

        lax.fori_loop(0, tokens // 8, body, 0)

    def synthesise(source, store):
        def body(chunk, carry):
            rows = pl.ds(pl.multiple_of(chunk * 8, 8), 8)
            terms = [(source[k, 0, rows, :], source[k, 1, rows, :]) for k in range(seq_count + 1)]
            for n, value in enumerate(real_from_half(terms, size, True)):
                store(n, rows, value)
            return carry

        lax.fori_loop(0, tokens // 8, body, 0)

    def across(tables, real, imag):
        both = three_dot(tables[0], tables[1], jnp.concatenate([real, imag], axis=0))
        return both[:tokens], both[tokens:]

    def convolve(batch, first):
        base = batch * seq_count
        analyse(lambda n, rows: recv[base + n, rows, :], spec)
        if first:
            analyse(lambda n, rows: taps_scr[n, rows, :], taps_spec)
        forward = (fwd_ref[0], fwd_ref[1])
        inverse = (inv_ref[0], inv_ref[1])

        def middle(k, carry):
            cosine, sine = tw_scr[k, 0], tw_scr[k, 1]
            real, imag = spec[k, 0], spec[k, 1]
            real, imag = real * cosine + imag * sine, imag * cosine - real * sine
            if first:
                tr, ti = taps_spec[k, 0], taps_spec[k, 1]
                tr, ti = tr * cosine + ti * sine, ti * cosine - tr * sine
                real, imag = across(forward, jnp.concatenate([real, tr], axis=1), jnp.concatenate([imag, ti], axis=1))
                h_r, h_i = real[:, LANES:], imag[:, LANES:]
                a_r, a_i = real[:, :LANES], imag[:, :LANES]
                h_i = jnp.where(left_mask(h_i.shape), h_i, -h_i)
                taps_spec[k, 0], taps_spec[k, 1] = h_r, h_i
            else:
                a_r, a_i = across(forward, real, imag)
                h_r, h_i = taps_spec[k, 0], taps_spec[k, 1]
            g_r, g_i = swap_halves(a_r), swap_halves(a_i)
            c_r, c_i = a_r * g_r + a_i * g_i, a_r * g_i - a_i * g_r
            p_r, p_i = a_r * h_r - a_i * h_i, a_r * h_i + a_i * h_r
            weight = jnp.where((k == 0) | (k == seq_count), 0.5 / (seq_count * tokens), 1.0 / (seq_count * tokens))
            cosine, sine = cosine * weight, sine * weight
            if first:
                corr_spec[k, 0], corr_spec[k, 1] = c_r, c_i
                br, bi = across(inverse, p_r, p_i)
            else:
                c_r, c_i = c_r + corr_spec[k, 0], c_i + corr_spec[k, 1]
                both_r, both_i = across(inverse, jnp.concatenate([p_r, c_r], axis=1), jnp.concatenate([p_i, c_i], axis=1))
                br, bi = both_r[:, :LANES], both_i[:, :LANES]
                cr, ci = both_r[:, LANES:], both_i[:, LANES:]
                corr_spec[k, 0] = cr * cosine - ci * sine
                corr_spec[k, 1] = ci * cosine + cr * sine
            spec[k, 0] = br * cosine - bi * sine
            spec[k, 1] = bi * cosine + br * sine
            return carry

        lax.fori_loop(0, seq_count + 1, middle, 0)

        def store(n, rows, value):
            result[base + n, rows, :] = value

        synthesise(spec, store)

    returning = [(result, back_recv, back_send_sem, back_recv_sem, False)]
    convolve(me_ch, True)
    leaving = exchange(returning, 0, *where_am_i)
    for copy in arriving[1]:
        copy.wait_recv()
    convolve(lax.rem(me_ch + 1, ch_count), False)
    leaving += exchange(returning, 1, *where_am_i)

    def store_corr(n, rows, value):
        corr_scr[n, rows, :] = value

    synthesise(corr_spec, store_corr)

    def gather_corr(block, carry):
        top = corr_scr[block, :half_tokens, :]
        bottom = swap_halves(corr_scr[block, half_tokens:, :])
        corr_result[block] = jnp.where(left_mask(top.shape), top, bottom) * scale
        return carry

    lax.fori_loop(0, seq_count, gather_corr, 0)
    last = exchange([(corr_result, corr_recv, corr_send_sem, corr_recv_sem, True)], 0, *where_am_i)
    back_recv[mine] = result[mine]
    corr_recv[me_seq] = corr_result[me_seq]
    for copy in leaving:
        copy.wait_recv()

    def finish(group, carry):
        lanes = pl.ds(pl.multiple_of(group * LANES, LANES), LANES)
        query_f = query_ref[:, lanes].astype(jnp.float32)
        key_f = key_ref[:, lanes].astype(jnp.float32)
        value_f = value_ref[:, lanes].astype(jnp.float32)
        out_f = out_ref[:, lanes].astype(jnp.float32)
        one, two = back_recv[2 * group], back_recv[2 * group + 1]
        left = left_mask(one.shape)
        skip = skip_ref[:, lanes]
        conv = jnp.where(left, one, swap_halves(two)) + skip * (key_f * value_f)
        back = jnp.where(left, swap_halves(one), two) + skip * (out_f * query_f)
        gq_ref[:, lanes] = (out_f * conv).astype(jnp.bfloat16)
        gk_ref[:, lanes] = (back * value_f).astype(jnp.bfloat16)
        gv_ref[:, lanes] = (back * key_f).astype(jnp.bfloat16)
        return carry

    lax.fori_loop(0, seq_count, finish, 0)
    for copy in last:
        copy.wait_recv()

    def finish_corr(group, carry):
        lanes = pl.ds(pl.multiple_of(group * LANES, LANES), LANES)
        one, two = corr_recv[2 * group], corr_recv[2 * group + 1]
        left = left_mask(one.shape)
        gf_ref[:half_tokens, lanes] = jnp.where(left, one, swap_halves(two))
        gf_ref[half_tokens:, lanes] = jnp.where(left, swap_halves(one), two)
        return carry

    lax.fori_loop(0, seq_count // 2, finish_corr, 0)
    for copy in arriving[0] + arriving[1] + leaving + last:
        copy.wait_send()


def tables(seq_count, tokens):
    index = np.arange(tokens)
    angle = 2.0 * np.pi / tokens * (index[:, None] * index[None, :] % tokens)
    cosine, sine = np.cos(angle), np.sin(angle)
    forward = np.block([[cosine, sine], [-sine, cosine]]).astype(np.float32)
    inverse = np.block([[cosine, -sine], [sine, cosine]]).astype(np.float32)

    def pieces(table):
        table = jnp.asarray(table)
        return jnp.stack(split_bf16(table))

    turn = 2.0 * np.pi / (2 * seq_count * tokens) * (np.arange(seq_count + 1)[:, None] * index[None, :])
    twiddle = jnp.asarray(np.stack([np.cos(turn).T, np.sin(turn).T]).astype(np.float32))
    return pieces(forward), pieces(inverse), twiddle


def fast_shards(query_gate, key_input, value_input, grad_output, filter_raw, skip_gain):
    seq_count, ch_count = lax.axis_size("seq"), lax.axis_size("ch")
    owners = seq_count * ch_count
    _, tokens, channels = key_input.shape
    vmem = pl.BlockSpec(memory_space=pltpu.VMEM)
    chunks = pltpu.VMEM((owners, tokens, LANES), jnp.float32)
    halves = pltpu.VMEM((seq_count, tokens // 2, LANES), jnp.float32)
    spectrum = pltpu.VMEM((seq_count + 1, 2, tokens, LANES), jnp.float32)
    lines = pltpu.VMEM((seq_count, tokens, LANES), jnp.float32)
    per_owner = pltpu.SemaphoreType.DMA((owners,))
    per_seq = pltpu.SemaphoreType.DMA((seq_count,))
    grads = pl.pallas_call(
        lambda *refs: layer_kernel(seq_count, ch_count, *refs),
        in_specs=[vmem] * 9,
        out_specs=[vmem] * 4,
        out_shape=[jax.ShapeDtypeStruct((tokens, channels), jnp.bfloat16)] * 3
        + [jax.ShapeDtypeStruct((tokens, channels // ch_count), jnp.float32)],
        scratch_shapes=[
            chunks, halves, chunks, halves, chunks, halves, chunks, halves,
            spectrum, spectrum, spectrum, lines, lines, spectrum,
            per_owner, per_owner, per_seq, per_seq, per_owner, per_owner, per_seq, per_seq,
        ],
        compiler_params=pltpu.CompilerParams(vmem_limit_bytes=VMEM_LIMIT, collective_id=0, has_side_effects=True),
        name="layer",
    )(query_gate[0], key_input[0], value_input[0], grad_output[0], filter_raw, skip_gain[None], *tables(seq_count, tokens))
    return (grads[0][None], grads[1][None], grads[2][None], grads[3])


def solution(mesh):
    in_specs = (
        P("ch", "seq", None),
        P("ch", "seq", None),
        P("ch", "seq", None),
        P("ch", "seq", None),
        P("seq", None),
        P(),
    )
    out_specs = (P("ch", "seq", None), P("ch", "seq", None), P("ch", "seq", None), P("seq", "ch"))

    def body(*arrays):
        seq_count, ch_count = mesh.shape["seq"], mesh.shape["ch"]
        _, tokens, channels = arrays[0].shape
        fits = ch_count == 2 and tokens == LANES and channels == seq_count * LANES and seq_count <= 32
        return (fast_shards if fits else shards)(*arrays)

    return jax.shard_map(body, mesh=mesh, in_specs=in_specs, out_specs=out_specs, check_vma=False)
```

```python
import math

import numpy as np

import jax
import jax.numpy as jnp
from jax import lax
from jax.experimental import pallas as pl
from jax.experimental.pallas import tpu as pltpu
from jax.sharding import PartitionSpec as P


def angle_table(row_index, col_index, modulus):
    turn_count = row_index[:, None] * col_index[None, :] % modulus
    angles = turn_count.astype(jnp.float32) * (2.0 * math.pi / modulus)
    return (jnp.cos(angles), jnp.sin(angles))


def contract(pattern, table, operand):
    return jnp.einsum(
        pattern, table, operand, precision=lax.Precision.HIGHEST, preferred_element_type=jnp.float32
    )


def rotate(pattern, cos_table, sin_table, sense_sign, real_part, imag_part, want_imag):
    if imag_part is None:
        cos_term = contract(pattern, cos_table, real_part)
        return (cos_term, sense_sign * contract(pattern, sin_table, real_part))
    real_out = contract(pattern, cos_table, real_part) - sense_sign * contract(
        pattern, sin_table, imag_part
    )
    if not want_imag:
        return (real_out, None)
    imag_out = contract(pattern, cos_table, imag_part) + sense_sign * contract(
        pattern, sin_table, real_part
    )
    return (real_out, imag_out)


def twist(cos_table, sin_table, sense_sign, real_part, imag_part):
    return (
        real_part * cos_table - sense_sign * imag_part * sin_table,
        imag_part * cos_table + sense_sign * real_part * sin_table,
    )


def spectral_terms(z_real, z_imag, g_real, g_imag, h_real, h_imag):
    conv_real = z_real * h_real - z_imag * h_imag
    conv_imag = z_real * h_imag + z_imag * h_real
    back_real = h_real * g_real + h_imag * g_imag
    back_imag = h_real * g_imag - h_imag * g_real
    corr_real = z_real * g_real + z_imag * g_imag
    corr_imag = z_real * g_imag - z_imag * g_real
    return (conv_real - back_imag, conv_imag + back_real, corr_real, corr_imag)


def shards(query_gate, key_input, value_input, grad_output, filter_raw, skip_gain):
    seq_count = lax.axis_size("seq")
    key_f = key_input[0].astype(jnp.float32)
    value_f = value_input[0].astype(jnp.float32)
    out_f = grad_output[0].astype(jnp.float32)
    mixed = key_f * value_f
    gated = out_f * query_gate[0].astype(jnp.float32)
    tokens, channels = mixed.shape
    seq_length = tokens * seq_count
    full_length = 2 * seq_length
    inverse_scale = 1.0 / full_length
    filter_taps = filter_raw.astype(jnp.float32) * seq_length ** (-0.5)
    freq_one = jnp.arange(2 * seq_count, dtype=jnp.int32)
    block_index = jnp.arange(seq_count, dtype=jnp.int32)
    offset_index = jnp.arange(tokens, dtype=jnp.int32)
    cos_one, sin_one = angle_table(freq_one, block_index, 2 * seq_count)
    cos_inv, sin_inv = angle_table(block_index, freq_one, 2 * seq_count)
    cos_two, sin_two = angle_table(offset_index, offset_index, tokens)
    local_width = channels // seq_count
    arrived = (
        lax.all_to_all(mixed.T, "seq", split_axis=0, concat_axis=1, tiled=True),
        lax.all_to_all(gated.T, "seq", split_axis=0, concat_axis=1, tiled=True),
        lax.all_to_all(filter_taps.T, "seq", split_axis=0, concat_axis=1, tiled=True),
    )
    cos_tw, sin_tw = angle_table(freq_one, offset_index, full_length)
    spectra = []
    for line_data in arrived:
        lines = line_data.reshape(local_width, seq_count, tokens)
        real_part, imag_part = rotate("kn,cnm->ckm", cos_one, sin_one, -1.0, lines, None, True)
        real_part, imag_part = twist(cos_tw, sin_tw, -1.0, real_part, imag_part)
        spectra.append(rotate("jm,ckm->ckj", cos_two, sin_two, -1.0, real_part, imag_part, True))
    packed_real, packed_imag, corr_real, corr_imag = spectral_terms(
        spectra[0][0], spectra[0][1], spectra[1][0], spectra[1][1], spectra[2][0], spectra[2][1]
    )
    pr_mid, pi_mid = rotate("mj,ckj->ckm", cos_two, sin_two, 1.0, packed_real, packed_imag, True)
    pr_mid, pi_mid = twist(cos_tw, sin_tw, 1.0, pr_mid, pi_mid)
    cr_mid, ci_mid = rotate("mj,ckj->ckm", cos_two, sin_two, 1.0, corr_real, corr_imag, True)
    cr_mid, ci_mid = twist(cos_tw, sin_tw, 1.0, cr_mid, ci_mid)
    conv_lines, back_lines = rotate("nk,ckm->cnm", cos_inv, sin_inv, 1.0, pr_mid, pi_mid, True)
    corr_lines = rotate("nk,ckm->cnm", cos_inv, sin_inv, 1.0, cr_mid, ci_mid, False)[0]
    conv_lines = (conv_lines * inverse_scale).reshape(local_width, seq_length)
    back_lines = (back_lines * inverse_scale).reshape(local_width, seq_length)
    corr_lines = (corr_lines * inverse_scale).reshape(local_width, seq_length)
    returned = (
        lax.all_to_all(conv_lines, "seq", split_axis=1, concat_axis=0, tiled=True),
        lax.all_to_all(back_lines, "seq", split_axis=1, concat_axis=0, tiled=True),
        lax.all_to_all(corr_lines, "seq", split_axis=1, concat_axis=0, tiled=True),
    )
    conv_time = returned[0].T
    back_time = returned[1].T
    corr_time = returned[2].T
    conv_full = conv_time + skip_gain * mixed
    back_full = back_time + skip_gain * gated
    grad_query = (out_f * conv_full).astype(jnp.bfloat16)[None]
    grad_key = (back_full * value_f).astype(jnp.bfloat16)[None]
    grad_value = (back_full * key_f).astype(jnp.bfloat16)[None]
    grad_filter = lax.psum_scatter(
        corr_time * seq_length ** (-0.5), "ch", scatter_dimension=1, tiled=True
    )
    return (grad_query, grad_key, grad_value, grad_filter)


LANES = 128
VMEM_LIMIT = 60 * 1024 * 1024


def times_root(pair, turn, size):
    real, imag = pair
    turn %= size
    if turn == 0:
        return pair
    if 4 * turn == size:
        return (-imag, real)
    if 2 * turn == size:
        return (-real, -imag)
    if 4 * turn == 3 * size:
        return (imag, -real)
    cosine = math.cos(2.0 * math.pi * turn / size)
    sine = math.sin(2.0 * math.pi * turn / size)
    return (real * cosine - imag * sine, real * sine + imag * cosine)


def complex_dft(values, sense):
    size = len(values)
    if size == 1:
        return values
    even = complex_dft(values[0::2], sense)
    odd = complex_dft(values[1::2], sense)
    low, high = [], []
    for k in range(size // 2):
        er, ei = even[k]
        tr, ti = times_root(odd[k], sense * k, size)
        low.append((er + tr, ei + ti))
        high.append((er - tr, ei - ti))
    return low + high


def half_spectrum(values, size):
    if size == 2:
        return [(values[0] + values[1], None), (values[0] - values[1], None)]
    half, quarter = size // 2, size // 4
    if len(values) == half:
        total, difference = values, values
    else:
        total = [values[n] + values[n + half] for n in range(half)]
        difference = [values[n] - values[n + half] for n in range(half)]
    out = [None] * (half + 1)
    out[0::2] = half_spectrum(total, half)
    turned = [times_root((difference[n], -difference[n + quarter]), -n, size) for n in range(quarter)]
    for index, (real, imag) in enumerate(complex_dft(turned, -1)):
        k = 1 + 4 * index
        if k <= half:
            out[k] = (real, imag)
        else:
            out[size - k] = (real, -imag)
    return out


def real_from_half(terms, size, first_half):
    if size == 2:
        return [terms[0][0] + terms[1][0], terms[0][0] - terms[1][0]]
    half, quarter = size // 2, size // 4
    even = real_from_half(terms[0::2], half, False)
    chosen = []
    for index in range(quarter):
        k = 1 + 4 * index
        if k <= half:
            chosen.append(terms[k])
        else:
            real, imag = terms[size - k]
            chosen.append((real, -imag))
    turned = [times_root(pair, n, size) for n, pair in enumerate(complex_dft(chosen, 1))]
    odd = [pair[0] for pair in turned] + [-pair[1] for pair in turned]
    out = [even[n] + odd[n] for n in range(half)]
    if first_half:
        return out
    return out + [even[n] - odd[n] for n in range(half)]


def split_bf16(value):
    high = value.astype(jnp.bfloat16)
    return high, (value - high.astype(jnp.float32)).astype(jnp.bfloat16)


def three_dot(table_high, table_low, value):
    high, low = split_bf16(value)
    dot = lambda a, b: jnp.dot(a, b, preferred_element_type=jnp.float32)
    return dot(table_high, high) + (dot(table_high, low) + dot(table_low, high))


def far_first(seq_count, ch_count):
    steps = sorted(range(seq_count), key=lambda step: abs(2 * step - seq_count))
    return [(step, turn) for step in steps for turn in range(ch_count) if step or turn]


def partner_of(step, turn, seq_count, ch_count, me_seq, me_ch):
    return {"seq": lax.rem(me_seq + step, seq_count), "ch": lax.rem(me_ch + turn, ch_count)}


def left_mask(shape):
    return lax.broadcasted_iota(jnp.int32, shape, 1) < LANES // 2


def swap_halves(value):
    return pltpu.roll(value, LANES // 2, 1)


def greet_all(seq_count, ch_count, me_seq, me_ch):
    barrier = pltpu.get_barrier_semaphore()
    for step, turn in far_first(seq_count, ch_count):
        pl.semaphore_signal(barrier, inc=1, device_id=partner_of(step, turn, seq_count, ch_count, me_seq, me_ch), device_id_type=pl.DeviceIdType.MESH)
    return barrier


def exchange(sends, turn, seq_count, ch_count, me_seq, me_ch):
    copies = []
    for step, at in far_first(seq_count, ch_count):
        if at != turn:
            continue
        partner = partner_of(step, turn, seq_count, ch_count, me_seq, me_ch)
        for source, target, send_sem, recv_sem, per_seq in sends:
            if per_seq:
                give, take, slot = partner["seq"], me_seq, step
            else:
                give, take, slot = partner["ch"] * seq_count + partner["seq"], me_ch * seq_count + me_seq, step * ch_count + turn
            copy = pltpu.make_async_remote_copy(
                src_ref=source.at[give],
                dst_ref=target.at[take],
                send_sem=send_sem.at[slot],
                recv_sem=recv_sem.at[slot],
                device_id=partner,
                device_id_type=pl.DeviceIdType.MESH,
            )
            copy.start()
            copies.append(copy)
    return copies


def layer_kernel(
    seq_count, ch_count,
    query_ref, key_ref, value_ref, out_ref, filter_ref, skip_ref, fwd_ref, inv_ref, tw_ref,
    gq_ref, gk_ref, gv_ref, gf_ref,
    send, taps_send, recv, taps_recv, result, corr_result, back_recv, corr_recv,
    spec, taps_spec, corr_spec, taps_scr, corr_scr, tw_scr,
    send_sem, recv_sem, taps_send_sem, taps_recv_sem, back_send_sem, back_recv_sem, corr_send_sem, corr_recv_sem,
):
    me_seq, me_ch = lax.axis_index("seq"), lax.axis_index("ch")
    where_am_i = (seq_count, ch_count, me_seq, me_ch)
    tokens, channels = key_ref.shape
    half_tokens = tokens // 2
    size = 2 * seq_count
    scale = (seq_count * tokens) ** -0.5
    own = me_ch * (channels // ch_count)
    mine = me_ch * seq_count + me_seq
    barrier = greet_all(*where_am_i)

    def prepare_taps(group, carry):
        lanes = pl.ds(pl.multiple_of(own + group * LANES, LANES), LANES)
        taps = filter_ref[:, lanes].astype(jnp.float32) * scale
        top, bottom = taps[:half_tokens], taps[half_tokens:]
        left = left_mask(top.shape)
        taps_send[2 * group] = jnp.where(left, top, swap_halves(bottom))
        taps_send[2 * group + 1] = jnp.where(left, swap_halves(top), bottom)
        return carry

    lax.fori_loop(0, seq_count // 2, prepare_taps, 0)

    pl.semaphore_wait(barrier, len(far_first(seq_count, ch_count)))
    arriving = [exchange([(taps_send, taps_recv, taps_send_sem, taps_recv_sem, True)], 0, *where_am_i)]

    def prepare(group, carry):
        lanes = pl.ds(pl.multiple_of(group * LANES, LANES), LANES)
        mixed = key_ref[:, lanes].astype(jnp.float32) * value_ref[:, lanes].astype(jnp.float32)
        gated = out_ref[:, lanes].astype(jnp.float32) * query_ref[:, lanes].astype(jnp.float32)
        left = left_mask(mixed.shape)
        send[2 * group] = jnp.where(left, mixed, swap_halves(gated))
        send[2 * group + 1] = jnp.where(left, swap_halves(mixed), gated)
        return carry

    groups = seq_count // ch_count
    first_group = me_ch * groups
    other_group = lax.rem(me_ch + 1, ch_count) * groups
    lax.fori_loop(first_group, first_group + groups, prepare, 0)
    arriving[0] += exchange([(send, recv, send_sem, recv_sem, False)], 0, *where_am_i)
    lax.fori_loop(other_group, other_group + groups, prepare, 0)
    arriving.append(exchange([(send, recv, send_sem, recv_sem, False)], 1, *where_am_i))
    recv[mine] = send[mine]
    taps_recv[me_seq] = taps_send[me_seq]
    for k in range(seq_count + 1):
        for part in range(2):
            tw_scr[k, part] = jnp.broadcast_to(tw_ref[part, :, k:k + 1], (tokens, LANES))
    for copy in arriving[0]:
        copy.wait_recv()

    def spread_taps(block, carry):
        packed = taps_recv[block]
        rolled = swap_halves(packed)
        left = left_mask(packed.shape)
        taps_scr[block, :half_tokens, :] = jnp.where(left, packed, rolled)
        taps_scr[block, half_tokens:, :] = jnp.where(left, rolled, packed)
        return carry

    lax.fori_loop(0, seq_count, spread_taps, 0)

    def analyse(load, target):
        def body(chunk, carry):
            rows = pl.ds(pl.multiple_of(chunk * 8, 8), 8)
            for k, (real, imag) in enumerate(half_spectrum([load(n, rows) for n in range(seq_count)], size)):
                target[k, 0, rows, :] = real
                target[k, 1, rows, :] = jnp.zeros_like(real) if imag is None else imag
            return carry

        lax.fori_loop(0, tokens // 8, body, 0)

    def synthesise(source, store):
        def body(chunk, carry):
            rows = pl.ds(pl.multiple_of(chunk * 8, 8), 8)
            terms = [(source[k, 0, rows, :], source[k, 1, rows, :]) for k in range(seq_count + 1)]
            for n, value in enumerate(real_from_half(terms, size, True)):
                store(n, rows, value)
            return carry

        lax.fori_loop(0, tokens // 8, body, 0)

    def across(tables, real, imag):
        both = three_dot(tables[0], tables[1], jnp.concatenate([real, imag], axis=0))
        return both[:tokens], both[tokens:]

    def convolve(batch, first):
        base = batch * seq_count
        analyse(lambda n, rows: recv[base + n, rows, :], spec)
        if first:
            analyse(lambda n, rows: taps_scr[n, rows, :], taps_spec)
        forward = (fwd_ref[0], fwd_ref[1])
        inverse = (inv_ref[0], inv_ref[1])

        def middle(k, carry):
            cosine, sine = tw_scr[k, 0], tw_scr[k, 1]
            real, imag = spec[k, 0], spec[k, 1]
            real, imag = real * cosine + imag * sine, imag * cosine - real * sine
            if first:
                tr, ti = taps_spec[k, 0], taps_spec[k, 1]
                tr, ti = tr * cosine + ti * sine, ti * cosine - tr * sine
                real, imag = across(forward, jnp.concatenate([real, tr], axis=1), jnp.concatenate([imag, ti], axis=1))
                h_r, h_i = real[:, LANES:], imag[:, LANES:]
                a_r, a_i = real[:, :LANES], imag[:, :LANES]
                h_i = jnp.where(left_mask(h_i.shape), h_i, -h_i)
                taps_spec[k, 0], taps_spec[k, 1] = h_r, h_i
            else:
                a_r, a_i = across(forward, real, imag)
                h_r, h_i = taps_spec[k, 0], taps_spec[k, 1]
            g_r, g_i = swap_halves(a_r), swap_halves(a_i)
            c_r, c_i = a_r * g_r + a_i * g_i, a_r * g_i - a_i * g_r
            p_r, p_i = a_r * h_r - a_i * h_i, a_r * h_i + a_i * h_r
            weight = jnp.where((k == 0) | (k == seq_count), 0.5 / (seq_count * tokens), 1.0 / (seq_count * tokens))
            cosine, sine = cosine * weight, sine * weight
            if first:
                corr_spec[k, 0], corr_spec[k, 1] = c_r, c_i
                br, bi = across(inverse, p_r, p_i)
            else:
                c_r, c_i = c_r + corr_spec[k, 0], c_i + corr_spec[k, 1]
                both_r, both_i = across(inverse, jnp.concatenate([p_r, c_r], axis=1), jnp.concatenate([p_i, c_i], axis=1))
                br, bi = both_r[:, :LANES], both_i[:, :LANES]
                cr, ci = both_r[:, LANES:], both_i[:, LANES:]
                corr_spec[k, 0] = cr * cosine - ci * sine
                corr_spec[k, 1] = ci * cosine + cr * sine
            spec[k, 0] = br * cosine - bi * sine
            spec[k, 1] = bi * cosine + br * sine
            return carry

        lax.fori_loop(0, seq_count + 1, middle, 0)

        def store(n, rows, value):
            result[base + n, rows, :] = value

        synthesise(spec, store)

    returning = [(result, back_recv, back_send_sem, back_recv_sem, False)]
    convolve(me_ch, True)
    leaving = [exchange(returning, 0, *where_am_i)]
    for copy in arriving[1]:
        copy.wait_recv()
    convolve(lax.rem(me_ch + 1, ch_count), False)
    leaving.append(exchange(returning, 1, *where_am_i))

    def store_corr(n, rows, value):
        corr_scr[n, rows, :] = value

    synthesise(corr_spec, store_corr)

    def gather_corr(block, carry):
        top = corr_scr[block, :half_tokens, :]
        bottom = swap_halves(corr_scr[block, half_tokens:, :])
        corr_result[block] = jnp.where(left_mask(top.shape), top, bottom) * scale
        return carry

    lax.fori_loop(0, seq_count, gather_corr, 0)
    last = exchange([(corr_result, corr_recv, corr_send_sem, corr_recv_sem, True)], 0, *where_am_i)
    back_recv[mine] = result[mine]
    corr_recv[me_seq] = corr_result[me_seq]

    def finish(group, carry):
        lanes = pl.ds(pl.multiple_of(group * LANES, LANES), LANES)
        query_f = query_ref[:, lanes].astype(jnp.float32)
        key_f = key_ref[:, lanes].astype(jnp.float32)
        value_f = value_ref[:, lanes].astype(jnp.float32)
        out_f = out_ref[:, lanes].astype(jnp.float32)
        one, two = back_recv[2 * group], back_recv[2 * group + 1]
        left = left_mask(one.shape)
        skip = skip_ref[:, lanes]
        conv = jnp.where(left, one, swap_halves(two)) + skip * (key_f * value_f)
        back = jnp.where(left, swap_halves(one), two) + skip * (out_f * query_f)
        gq_ref[:, lanes] = (out_f * conv).astype(jnp.bfloat16)
        gk_ref[:, lanes] = (back * value_f).astype(jnp.bfloat16)
        gv_ref[:, lanes] = (back * key_f).astype(jnp.bfloat16)
        return carry

    for copy in leaving[0]:
        copy.wait_recv()
    lax.fori_loop(first_group, first_group + groups, finish, 0)
    for copy in leaving[1]:
        copy.wait_recv()
    lax.fori_loop(other_group, other_group + groups, finish, 0)
    for copy in last:
        copy.wait_recv()

    def finish_corr(group, carry):
        lanes = pl.ds(pl.multiple_of(group * LANES, LANES), LANES)
        one, two = corr_recv[2 * group], corr_recv[2 * group + 1]
        left = left_mask(one.shape)
        gf_ref[:half_tokens, lanes] = jnp.where(left, one, swap_halves(two))
        gf_ref[half_tokens:, lanes] = jnp.where(left, swap_halves(one), two)
        return carry

    lax.fori_loop(0, seq_count // 2, finish_corr, 0)
    for copy in arriving[0] + arriving[1] + leaving[0] + leaving[1] + last:
        copy.wait_send()


def tables(seq_count, tokens):
    index = np.arange(tokens)
    angle = 2.0 * np.pi / tokens * (index[:, None] * index[None, :] % tokens)
    cosine, sine = np.cos(angle), np.sin(angle)
    forward = np.block([[cosine, sine], [-sine, cosine]]).astype(np.float32)
    inverse = np.block([[cosine, -sine], [sine, cosine]]).astype(np.float32)

    def pieces(table):
        table = jnp.asarray(table)
        return jnp.stack(split_bf16(table))

    turn = 2.0 * np.pi / (2 * seq_count * tokens) * (np.arange(seq_count + 1)[:, None] * index[None, :])
    twiddle = jnp.asarray(np.stack([np.cos(turn).T, np.sin(turn).T]).astype(np.float32))
    return pieces(forward), pieces(inverse), twiddle


def fast_shards(query_gate, key_input, value_input, grad_output, filter_raw, skip_gain):
    seq_count, ch_count = lax.axis_size("seq"), lax.axis_size("ch")
    owners = seq_count * ch_count
    _, tokens, channels = key_input.shape
    vmem = pl.BlockSpec(memory_space=pltpu.VMEM)
    chunks = pltpu.VMEM((owners, tokens, LANES), jnp.float32)
    halves = pltpu.VMEM((seq_count, tokens // 2, LANES), jnp.float32)
    spectrum = pltpu.VMEM((seq_count + 1, 2, tokens, LANES), jnp.float32)
    lines = pltpu.VMEM((seq_count, tokens, LANES), jnp.float32)
    per_owner = pltpu.SemaphoreType.DMA((owners,))
    per_seq = pltpu.SemaphoreType.DMA((seq_count,))
    grads = pl.pallas_call(
        lambda *refs: layer_kernel(seq_count, ch_count, *refs),
        in_specs=[vmem] * 9,
        out_specs=[vmem] * 4,
        out_shape=[jax.ShapeDtypeStruct((tokens, channels), jnp.bfloat16)] * 3
        + [jax.ShapeDtypeStruct((tokens, channels // ch_count), jnp.float32)],
        scratch_shapes=[
            chunks, halves, chunks, halves, chunks, halves, chunks, halves,
            spectrum, spectrum, spectrum, lines, lines, spectrum,
            per_owner, per_owner, per_seq, per_seq, per_owner, per_owner, per_seq, per_seq,
        ],
        compiler_params=pltpu.CompilerParams(vmem_limit_bytes=VMEM_LIMIT, collective_id=0, has_side_effects=True),
        name="layer",
    )(query_gate[0], key_input[0], value_input[0], grad_output[0], filter_raw, skip_gain[None], *tables(seq_count, tokens))
    return (grads[0][None], grads[1][None], grads[2][None], grads[3])


def solution(mesh):
    in_specs = (
        P("ch", "seq", None),
        P("ch", "seq", None),
        P("ch", "seq", None),
        P("ch", "seq", None),
        P("seq", None),
        P(),
    )
    out_specs = (P("ch", "seq", None), P("ch", "seq", None), P("ch", "seq", None), P("seq", "ch"))

    def body(*arrays):
        seq_count, ch_count = mesh.shape["seq"], mesh.shape["ch"]
        _, tokens, channels = arrays[0].shape
        fits = ch_count == 2 and tokens == LANES and channels == seq_count * LANES and seq_count <= 32
        return (fast_shards if fits else shards)(*arrays)

    return jax.shard_map(body, mesh=mesh, in_specs=in_specs, out_specs=out_specs, check_vma=False)
```
